8 devices in a mesh: stage: 2 (over z, y), expert: 4 (over x, core).
Axes of the slice: x: 2, y: 2, z: 1, core: 2. Of those that a mesh axis runs over, the one named last changes fastest.
Arguments:
- x_act: bfloat16 [2, 4096, 2048], P('stage', 'expert')
- route_idx: int32 [2, 4096, 2], P('stage', 'expert')
- route_gate: float32 [2, 4096, 2], P('stage', 'expert')
- w_up: bfloat16 [2, 16, 2048, 1024], P('stage', 'expert')
- w_lin: bfloat16 [2, 16, 2048, 1024], P('stage', 'expert')
- w_down: bfloat16 [2, 16, 1024, 2048], P('stage', 'expert')
- dy_out: bfloat16 [2, 4096, 2048], P('stage', 'expert')
Outputs:
- output 1: bfloat16 [2, 4096, 2048], P('stage', 'expert')
- output 2: bfloat16 [2, 4096, 2048], P('stage', 'expert')
- output 3: bfloat16 [2, 16, 2048, 1024], P('stage', 'expert')
- output 4: bfloat16 [2, 16, 2048, 1024], P('stage', 'expert')
- output 5: bfloat16 [2, 16, 1024, 2048], P('stage', 'expert')
All inputs are finite; a program needn't handle non-finite values.
Results may differ from the reference program's by a relative error of at most 0.00122.
Values are sent between devices in bfloat16 or wider.
A program may use at most 1 GiB of HBM per device.

```python
import jax
import jax.numpy as jnp
from jax import lax

STAGE_DEVS = 2
EXPERT_DEVS = 4
TOKENS = 1024
D_MODEL = 2048
D_FF = 1024
EXPERTS = 16
TOP_K = 2

CAPACITY = 4 * TOKENS // EXPERTS
ROWS = EXPERT_DEVS * TOKENS


def draw_routing(rng_key):
    key_hot, key_bias, key_cell, key_perm, key_swap = jax.random.split(rng_key, 5)
    num_cells = EXPERTS * CAPACITY
    cell_ids = jnp.arange(num_cells, dtype=jnp.int32)
    cell_expert = cell_ids // CAPACITY
    cell_slot = cell_ids % CAPACITY
    hot_expert = jax.random.randint(key_hot, (), 0, EXPERTS)
    expert_bias = jax.random.randint(key_bias, (EXPERTS,), 0, 4) * 256
    cell_score = jax.random.randint(key_cell, (num_cells,), 0, 1024) + expert_bias[cell_expert]
    needed = (cell_slot == 0) | (cell_expert == hot_expert)
    cell_score = jnp.where(needed, 4096, cell_score)
    top_vals, chosen = lax.top_k(cell_score * num_cells + cell_ids, 2 * TOKENS)
    chosen_expert = jnp.sort(chosen) // CAPACITY
    expert_pairs = jnp.stack([chosen_expert[:TOKENS], chosen_expert[TOKENS:]], axis=1)
    expert_pairs = expert_pairs[jax.random.permutation(key_perm, TOKENS)]
    swap_flag = jax.random.randint(key_swap, (TOKENS, 1), 0, 2)
    return jnp.where(swap_flag == 1, expert_pairs[:, ::-1], expert_pairs).astype(jnp.int32)


def setup_inputs(seed: int = 0) -> dict:
    root_key = jax.random.key(seed)
    key_x, key_route, key_gate, key_up, key_lin, key_down, key_dy = jax.random.split(root_key, 7)
    shape_tok = (STAGE_DEVS, ROWS, D_MODEL)
    x_act = jax.random.normal(key_x, shape_tok, jnp.float32).astype(jnp.bfloat16)
    route_keys = jax.random.split(key_route, STAGE_DEVS * EXPERT_DEVS)
    route_idx = jax.vmap(draw_routing)(route_keys).reshape(STAGE_DEVS, ROWS, TOP_K)
    first_gate = jax.random.uniform(key_gate, (STAGE_DEVS, ROWS, 1), jnp.float32, 0.3, 0.7)
    route_gate = jnp.concatenate([first_gate, 1.0 - first_gate], axis=-1)
    shape_in = (STAGE_DEVS, EXPERTS, D_MODEL, D_FF)
    shape_out = (STAGE_DEVS, EXPERTS, D_FF, D_MODEL)
    w_up = (jax.random.normal(key_up, shape_in, jnp.float32) * D_MODEL ** -0.5).astype(jnp.bfloat16)
    w_lin = (jax.random.normal(key_lin, shape_in, jnp.float32) * D_MODEL ** -0.5).astype(jnp.bfloat16)
    w_down = (jax.random.normal(key_down, shape_out, jnp.float32) * D_FF ** -0.5).astype(jnp.bfloat16)
    dy_out = jax.random.normal(key_dy, shape_tok, jnp.float32).astype(jnp.bfloat16)
    return {"x_act": x_act, "route_idx": route_idx, "route_gate": route_gate, "w_up": w_up, "w_lin": w_lin, "w_down": w_down, "dy_out": dy_out}


def expert_block(x_src, idx_src, gate_src, dy_dst, w_up, w_lin, w_down):
    member = jnp.sum(jax.nn.one_hot(idx_src, EXPERTS, dtype=jnp.int32), axis=1)
    earlier = jnp.cumsum(member, axis=0) - member
    slot_pos = jnp.take_along_axis(earlier, idx_src, axis=1)
    x_copies = jnp.broadcast_to(x_src.astype(jnp.float32)[:, None, :], (TOKENS, TOP_K, D_MODEL))
    empty_rows = jnp.zeros((EXPERTS, CAPACITY, D_MODEL), jnp.float32)
    x_rows = empty_rows.at[idx_src, slot_pos].set(x_copies)
    pre_up = jnp.einsum("ecd,edf->ecf", x_rows, w_up)
    pre_lin = jnp.einsum("ecd,edf->ecf", x_rows, w_lin)
    act_up = jax.nn.silu(pre_up)
    hidden = (act_up * pre_lin).astype(jnp.bfloat16).astype(jnp.float32)
    out_rows = jnp.einsum("ecf,efd->ecd", hidden, w_down).astype(jnp.bfloat16).astype(jnp.float32)
    out_copies = out_rows[idx_src, slot_pos]
    y_tok = jnp.sum(gate_src[:, :, None] * out_copies, axis=1).astype(jnp.bfloat16)
    d_copies = (gate_src[:, :, None] * dy_dst.astype(jnp.float32)[:, None, :]).astype(jnp.bfloat16).astype(jnp.float32)
    d_rows = empty_rows.at[idx_src, slot_pos].set(d_copies)
    d_hidden = jnp.einsum("ecd,efd->ecf", d_rows, w_down).astype(jnp.bfloat16).astype(jnp.float32)
    sigmoid_up = jax.nn.sigmoid(pre_up)
    d_up = (d_hidden * pre_lin * sigmoid_up * (1.0 + pre_up * (1.0 - sigmoid_up))).astype(jnp.bfloat16).astype(jnp.float32)
    d_lin = (d_hidden * act_up).astype(jnp.bfloat16).astype(jnp.float32)
    g_up = jnp.einsum("ecd,ecf->edf", x_rows, d_up)
    g_lin = jnp.einsum("ecd,ecf->edf", x_rows, d_lin)
    g_down = jnp.einsum("ecf,ecd->efd", hidden, d_rows)
    dx_rows = (jnp.einsum("ecf,edf->ecd", d_up, w_up) + jnp.einsum("ecf,edf->ecd", d_lin, w_lin)).astype(jnp.bfloat16).astype(jnp.float32)
    dx_tok = jnp.sum(dx_rows[idx_src, slot_pos], axis=1).astype(jnp.bfloat16)
    return y_tok, dx_tok, g_up, g_lin, g_down


def stage_block(stage_args):
    x_stage, idx_stage, gate_stage, dy_stage, w_up, w_lin, w_down = stage_args
    w_up32 = w_up.astype(jnp.float32)
    w_lin32 = w_lin.astype(jnp.float32)
    w_down32 = w_down.astype(jnp.float32)

    def device_step(grad_sums, dev_block):
        block_out = expert_block(dev_block[0], dev_block[1], dev_block[2], dev_block[3], w_up32, w_lin32, w_down32)
        new_sums = (grad_sums[0] + block_out[2], grad_sums[1] + block_out[3], grad_sums[2] + block_out[4])
        return new_sums, (block_out[0], block_out[1])

    zero_grads = (jnp.zeros((EXPERTS, D_MODEL, D_FF), jnp.float32), jnp.zeros((EXPERTS, D_MODEL, D_FF), jnp.float32), jnp.zeros((EXPERTS, D_FF, D_MODEL), jnp.float32))
    dev_blocks = (x_stage.reshape(EXPERT_DEVS, TOKENS, D_MODEL), idx_stage.reshape(EXPERT_DEVS, TOKENS, TOP_K), gate_stage.reshape(EXPERT_DEVS, TOKENS, TOP_K), dy_stage.reshape(EXPERT_DEVS, TOKENS, D_MODEL))
    grad_sums, tok_outs = lax.scan(device_step, zero_grads, dev_blocks)
    y_stage = tok_outs[0].reshape(ROWS, D_MODEL)
    dx_stage = tok_outs[1].reshape(ROWS, D_MODEL)
    return y_stage, dx_stage, grad_sums[0].astype(jnp.bfloat16), grad_sums[1].astype(jnp.bfloat16), grad_sums[2].astype(jnp.bfloat16)


def reference(x_act, route_idx, route_gate, w_up, w_lin, w_down, dy_out):
    x_from = jnp.roll(x_act, 1, axis=0)
    idx_from = jnp.roll(route_idx, 1, axis=0)
    gate_from = jnp.roll(route_gate, 1, axis=0)
    y_out, dx_next, dw_up, dw_lin, dw_down = lax.map(stage_block, (x_from, idx_from, gate_from, dy_out, w_up, w_lin, w_down))
    dx_act = jnp.roll(dx_next, -1, axis=0)
    return y_out, dx_act, dw_up, dw_lin, dw_down
```

```python
import functools

import jax
import jax.numpy as jnp
from jax import lax
from jax.experimental import pallas as pl
from jax.experimental.pallas import tpu as pltpu
from jax.sharding import PartitionSpec as P


F32 = jnp.float32
BF16 = jnp.bfloat16
NT = (((1,), (1,)), ((), ()))
TN = (((0,), (0,)), ((), ()))


def mm(a, b, dims=(((1,), (0,)), ((), ()))):
    return lax.dot_general(a, b, dims, preferred_element_type=F32)


def call(body, grid, in_specs, out_specs, out_shape, args, flops, scratch=()):
    nbytes = sum(a.size * a.dtype.itemsize for a in args)
    return pl.pallas_call(
        body, grid=grid, in_specs=in_specs, out_specs=out_specs, out_shape=out_shape,
        scratch_shapes=list(scratch),
        cost_estimate=pl.CostEstimate(flops=flops, bytes_accessed=nbytes, transcendentals=0),
        compiler_params=pltpu.CompilerParams(dimension_semantics=("arbitrary",) * len(grid)),
    )(*args)


def spec(block, index):
    return pl.BlockSpec(block, index)


def dispatch_body(*refs, sizes, scale):
    count = sum(len(per) for per in sizes)
    pos_ref, gate_ref = refs[:2]
    chunks, (out_ref, hit_ref, scale_ref) = refs[2:2 + count], refs[2 + count:]
    num_exp, cap = out_ref.shape[0], out_ref.shape[1] // 2
    tokens = pos_ref.shape[3]

    @pl.when(pl.program_id(0) == 0)
    def _():
        slot = lax.broadcasted_iota(jnp.int32, (cap, tokens), 0)
        for s in range(2):
            for e in range(num_exp):
                hit = pos_ref[s, e] == slot
                hit_ref[s, e * cap:(e + 1) * cap, :] = hit.astype(BF16)
                if scale:
                    scale_ref[s, e * cap:(e + 1) * cap, :] = jnp.sum(jnp.where(hit, gate_ref[s, e], 0.0), axis=1, keepdims=True)

    at = 0
    for s, per in enumerate(sizes):
        rows, first = None, 0
        for size in per:
            part = mm(hit_ref[s][:, first:first + size], chunks[at][...])
            rows = part if rows is None else rows + part
            first, at = first + size, at + 1
        if scale:
            rows = rows * scale_ref[s]
        rows = rows.astype(BF16)
        for e in range(num_exp):
            out_ref[e, s * cap:(s + 1) * cap, :] = rows[e * cap:(e + 1) * cap]


def dispatch(pos, gate, blocks, cap, scale):
    _, num_exp, _, tokens = pos.shape
    chunks = [c for blk in blocks for c in blk]
    sizes = tuple(tuple(c.shape[0] for c in blk) for blk in blocks)
    width = chunks[0].shape[1]
    dt = 512
    row = spec(pos.shape, lambda d: (0, 0, 0, 0))
    toks = [spec((c.shape[0], dt), lambda d: (0, d)) for c in chunks]
    return call(functools.partial(dispatch_body, sizes=sizes, scale=scale), (width // dt,), [row, row] + toks,
                spec((num_exp, 2 * cap, dt), lambda d: (0, 0, d)),
                jax.ShapeDtypeStruct((num_exp, 2 * cap, width), BF16), (pos, gate, *chunks),
                4 * cap * tokens * width * num_exp,
                [pltpu.VMEM((2, num_exp * cap, tokens), BF16), pltpu.VMEM((2, num_exp * cap, 1), F32)])


def forward_body(x_ref, wu_ref, wl_ref, a_ref, b_ref, h_ref):
    a = mm(x_ref[0], wu_ref[0])
    b = mm(x_ref[0], wl_ref[0])
    a_ref[0] = a
    b_ref[0] = b
    h_ref[0] = (jax.nn.silu(a) * b).astype(BF16)


def forward(x_rows, w_up, w_lin):
    num_exp, rows, width = x_rows.shape
    ff = w_up.shape[2]
    ft = 512
    w = spec((1, width, ft), lambda e, f: (e, 0, f))
    o = spec((1, rows, ft), lambda e, f: (e, 0, f))
    full = functools.partial(jax.ShapeDtypeStruct, (num_exp, rows, ff))
    return call(forward_body, (num_exp, ff // ft), [spec((1, rows, width), lambda e, f: (e, 0, 0)), w, w], [o, o, o],
                [full(F32), full(F32), full(BF16)], (x_rows, w_up, w_lin), 4 * num_exp * rows * width * ff)


def act_grads(a, b, dh):
    sig = jax.nn.sigmoid(a)
    d_up = (dh * b * sig * (1.0 + a * (1.0 - sig))).astype(BF16)
    d_lin = (dh * (a * sig)).astype(BF16)
    return d_up, d_lin


def backward_body(u_ref, wd_ref, a_ref, b_ref, da_ref, db_ref):
    dh = mm(u_ref[0], wd_ref[0], NT).astype(BF16).astype(F32)
    da_ref[0], db_ref[0] = act_grads(a_ref[0], b_ref[0], dh)


def backward(u_rows, w_down, a, b):
    num_exp, rows, width = u_rows.shape
    ff = w_down.shape[1]
    ft = 512
    o = spec((1, rows, ft), lambda e, f: (e, 0, f))
    full = jax.ShapeDtypeStruct((num_exp, rows, ff), BF16)
    return call(backward_body, (num_exp, ff // ft),
                [spec((1, rows, width), lambda e, f: (e, 0, 0)), spec((1, ft, width), lambda e, f: (e, f, 0)), o, o], [o, o],
                [full, full], (u_rows, w_down, a, b), 2 * num_exp * rows * width * ff)


def both_body(x_ref, u_ref, wu_ref, wl_ref, wd_ref, h_ref, da_ref, db_ref):
    a = mm(x_ref[0], wu_ref[0])
    b = mm(x_ref[0], wl_ref[0])
    h_ref[0] = (jax.nn.silu(a) * b).astype(BF16)
    dh = mm(u_ref[0], wd_ref[0], NT).astype(BF16).astype(F32)
    da_ref[0], db_ref[0] = act_grads(a, b, dh)


def both(x_rows, u_rows, w_up, w_lin, w_down):
    num_exp, rows, width = x_rows.shape
    ff = w_up.shape[2]
    ft = 512
    r = spec((1, rows, width), lambda e, f: (e, 0, 0))
    w = spec((1, width, ft), lambda e, f: (e, 0, f))
    o = spec((1, rows, ft), lambda e, f: (e, 0, f))
    full = jax.ShapeDtypeStruct((num_exp, rows, ff), BF16)
    return call(both_body, (num_exp, ff // ft), [r, r, w, w, spec((1, ft, width), lambda e, f: (e, f, 0))], [o, o, o],
                [full, full, full], (x_rows, u_rows, w_up, w_lin, w_down), 6 * num_exp * rows * width * ff)


def out_body(two_ref, pos_ref, coef_ref, h_ref, wd_ref, ya_ref, yb_ref, place_ref, rows_ref):
    num_exp, rows, _ = h_ref.shape
    cap = rows // 2
    tokens = ya_ref.shape[0]

    def build(s, j):
        slot = lax.broadcasted_iota(jnp.int32, (tokens, cap), 1)
        for e in range(num_exp):
            at = pos_ref[s][:, j * num_exp + e:j * num_exp + e + 1]
            place_ref[s, j * tokens:(j + 1) * tokens, e * cap:(e + 1) * cap] = (at == slot).astype(BF16)

    @pl.when(pl.program_id(0) == 0)
    def _():
        for s in range(2):
            build(s, 0)
            pl.when(two_ref[s] > 0)(functools.partial(build, s, 1))

    for e in range(num_exp):
        o = mm(h_ref[e], wd_ref[e]).astype(BF16)
        for s in range(2):
            rows_ref[s, e * cap:(e + 1) * cap, :] = o[s * cap:(s + 1) * cap]
    for s, y_ref in enumerate((ya_ref, yb_ref)):

        @pl.when(two_ref[s] == 0)
        def _():
            y_ref[...] = mm(place_ref[s, :tokens], rows_ref[s]).astype(BF16)

        @pl.when(two_ref[s] > 0)
        def _():
            first = coef_ref[s][:, 0:1] * mm(place_ref[s, :tokens], rows_ref[s])
            y_ref[...] = (first + coef_ref[s][:, 1:2] * mm(place_ref[s, tokens:], rows_ref[s])).astype(BF16)


def out_rows(two, pos, coef, hidden, w_down, part, parts):
    _, tokens, _ = pos.shape
    num_exp, rows, ff = hidden.shape
    width = w_down.shape[2] // parts
    dt = 256
    first = part * (width // dt)
    whole = lambda arr: spec(arr.shape, lambda d: (0,) * arr.ndim)
    o = spec((tokens, dt), lambda d: (0, d))
    full = jax.ShapeDtypeStruct((tokens, width), BF16)
    return call(out_body, (width // dt,),
                [pl.BlockSpec(memory_space=pltpu.SMEM), whole(pos), whole(coef), whole(hidden),
                 spec((num_exp, ff, dt), lambda d: (0, 0, first + d))], [o, o],
                [full, full], (two, pos, coef, hidden, w_down),
                2 * num_exp * rows * ff * width + 8 * tokens * num_exp * (rows // 2) * width,
                [pltpu.VMEM((2, 2 * tokens, num_exp * (rows // 2)), BF16), pltpu.VMEM((2, num_exp * (rows // 2), dt), BF16)])


def dx_body(pos_ref, da_ref, db_ref, wu_ref, wl_ref, ya_ref, yb_ref, place_ref, rows_ref):
    num_exp, rows, _ = da_ref.shape
    cap = rows // 2
    tokens = ya_ref.shape[0]

    @pl.when(pl.program_id(0) == 0)
    def _():
        slot = lax.broadcasted_iota(jnp.int32, (tokens, cap), 1)
        for s in range(2):
            for e in range(num_exp):
                at = pos_ref[s][:, e:e + 1]
                place_ref[s, :, e * cap:(e + 1) * cap] = (at == slot).astype(BF16)

    for e in range(num_exp):
        o = (mm(da_ref[e], wu_ref[e], NT) + mm(db_ref[e], wl_ref[e], NT)).astype(BF16)
        for s in range(2):
            rows_ref[s, e * cap:(e + 1) * cap, :] = o[s * cap:(s + 1) * cap]
    for s, y_ref in enumerate((ya_ref, yb_ref)):
        y_ref[...] = mm(place_ref[s], rows_ref[s]).astype(BF16)


def dx_rows(pos, d_up, d_lin, w_up, w_lin, part, parts):
    _, tokens, _ = pos.shape
    num_exp, rows, ff = d_up.shape
    width = w_up.shape[1] // parts
    dt = 256
    first = part * (width // dt)
    whole = lambda arr: spec(arr.shape, lambda d: (0,) * arr.ndim)
    w = spec((num_exp, dt, ff), lambda d: (0, first + d, 0))
    o = spec((tokens, dt), lambda d: (0, d))
    full = jax.ShapeDtypeStruct((tokens, width), BF16)
    return call(dx_body, (width // dt,), [whole(pos), whole(d_up), whole(d_lin), w, w], [o, o],
                [full, full], (pos, d_up, d_lin, w_up, w_lin),
                4 * num_exp * rows * ff * width + 4 * tokens * num_exp * (rows // 2) * width,
                [pltpu.VMEM((2, tokens, num_exp * (rows // 2)), BF16), pltpu.VMEM((2, num_exp * (rows // 2), dt), BF16)])


def grads_in_body(xh_ref, xr_ref, ah_ref, ar_ref, bh_ref, br_ref, gu_ref, gl_ref):
    gu_ref[0] = (mm(xh_ref[0], ah_ref[0], TN) + mm(xr_ref[0], ar_ref[0], TN)).astype(BF16)
    gl_ref[0] = (mm(xh_ref[0], bh_ref[0], TN) + mm(xr_ref[0], br_ref[0], TN)).astype(BF16)


def grads_in(x_home, x_rem, da_h, da_r, db_h, db_r):
    num_exp, rows, width = x_home.shape
    ff = da_h.shape[2]
    mt = 1024
    x = spec((1, rows, mt), lambda e, m: (e, 0, m))
    d = spec((1, rows, ff), lambda e, m: (e, 0, 0))
    o = spec((1, mt, ff), lambda e, m: (e, m, 0))
    full = jax.ShapeDtypeStruct((num_exp, width, ff), BF16)
    return call(grads_in_body, (num_exp, width // mt), [x, x, d, d, d, d], [o, o], [full, full],
                (x_home, x_rem, da_h, da_r, db_h, db_r), 8 * num_exp * rows * width * ff)


def grad_down_body(hh_ref, hr_ref, uh_ref, ur_ref, g_ref):
    g_ref[0] = (mm(hh_ref[0], uh_ref[0], TN) + mm(hr_ref[0], ur_ref[0], TN)).astype(BF16)


def grad_down(h_home, h_rem, u_home, u_rem):
    num_exp, rows, ff = h_home.shape
    width = u_home.shape[2]
    mt = 512
    h = spec((1, rows, mt), lambda e, m: (e, 0, m))
    u = spec((1, rows, width), lambda e, m: (e, 0, 0))
    return call(grad_down_body, (num_exp, ff // mt), [h, h, u, u], spec((1, mt, width), lambda e, m: (e, m, 0)),
                jax.ShapeDtypeStruct((num_exp, ff, width), BF16), (h_home, h_rem, u_home, u_rem), 4 * num_exp * rows * width * ff)


def merge_body(*refs, halves, scaled):
    out_ref = refs[-1]
    coef_ref = refs[0] if scaled else None
    ins = list(refs[1:-1] if scaled else refs[:-1])
    width = out_ref.shape[1] // halves
    for k in range(halves):
        total = None
        for n, h in enumerate((1,) * (len(ins) - halves + 1) if halves > 1 else (1,) * len(ins)):
            ref = ins[n + k] if halves > 1 and n == len(ins) - halves else ins[n]
            val = ref[:, k * width:(k + 1) * width] if ref.shape[1] > width else ref[...]
            val = val.astype(F32)
            if scaled:
                val = coef_ref[:, n:n + 1] * val
            total = val if total is None else total + val
        out_ref[:, k * width:(k + 1) * width] = total.astype(BF16)


def merge(arrs, width, part=0, coef=None, halves=1):
    tokens = arrs[0].shape[0]
    rt = 256
    specs = [] if coef is None else [spec((rt, coef.shape[1]), lambda i: (i, 0))]
    for arr in arrs:
        cols = min(arr.shape[1], width)
        specs.append(spec((rt, cols), (lambda i: (i, part)) if arr.shape[1] > cols else (lambda i: (i, 0))))
    args = tuple(arrs) if coef is None else (coef, *arrs)
    return call(functools.partial(merge_body, halves=halves, scaled=coef is not None), (tokens // rt,), specs,
                spec((rt, width), lambda i: (i, 0)), jax.ShapeDtypeStruct((tokens, width), BF16), args, 2 * len(arrs) * tokens * width)


def solution(mesh):
    stages = mesh.shape["stage"]
    groups = mesh.shape["expert"]
    ndev = stages * groups
    tok_spec = P("stage", "expert", None)
    w_spec = P("stage", "expert", None, None)

    def move(arr, step, flip):
        pairs = [(d, ((d // groups + step) % stages) * groups + ((d % groups) ^ flip)) for d in range(ndev)]
        return lax.ppermute(arr, ("stage", "expert"), pairs)

    def device_step(x_act, route_idx, route_gate, w_up, w_lin, w_down, dy_out):
        tokens, width = x_act.shape[1:]
        local_exp = w_up.shape[1]
        num_experts = local_exp * groups
        cap = 4 * tokens // num_experts
        w_up, w_lin, w_down = w_up[0], w_lin[0], w_down[0]
        me = lax.axis_index("expert")

        meta = jnp.concatenate([route_idx[0].astype(F32).T, route_gate[0].T], axis=0)
        metas = jnp.stack([move(meta, 1, flip) for flip in range(groups)])
        ids = metas[:, :2].astype(jnp.int32)
        gates = metas[:, 2:]

        nc = 4
        rows = tokens // nc
        d_own = dy_out[0]
        d_par = move(d_own, 0, 1)
        d_x = [move(d_own[:rows], 0, 2), move(d_own[rows:], 0, 2)]
        d_o = [move(c, 0, 1) for c in d_x]
        x_y = [move(x_act[0, k * rows:(k + 1) * rows], 1, 0) for k in range(nc)]
        x_x = [move(c, 0, 2) for c in x_y]
        x_p = [move(c, 0, 1) for c in x_y]
        x_o = [move(c, 0, 1) for c in x_x]

        exp_ids = me * local_exp + jnp.arange(local_exp, dtype=jnp.int32)
        hit = ids[:, :, None, :] == exp_ids[None, None, :, None]
        member = jnp.any(hit, axis=1)
        lower = (jnp.arange(tokens)[:, None] < jnp.arange(tokens)[None, :]).astype(BF16)
        before = jnp.dot(member.reshape(-1, tokens).astype(BF16), lower, preferred_element_type=F32).astype(jnp.int32).reshape(member.shape)
        pos = jnp.where(member, before, -1)[:, :, None, :]
        sel_gate = jnp.sum(jnp.where(hit, gates[:, :, None, :], 0.0), axis=1)[:, :, None, :]
        here = (ids // local_exp) == me
        there = (ids // local_exp) == (me ^ 1)
        cnt = jnp.sum(here.astype(jnp.int32), axis=1)
        cnt_p = jnp.sum(there.astype(jnp.int32), axis=1)
        two = jnp.sum((cnt == 2).astype(jnp.int32), axis=1)
        both_here = (cnt == 2)[:, None, :]
        pos_any = jnp.where(member, before, -1)
        pos_first = jnp.where(both_here & ~hit[:, 0], -1, pos_any)
        pos_second = jnp.where(both_here & hit[:, 1], before, -1)
        pos_tok = jnp.concatenate([pos_first, pos_second], axis=1).transpose(0, 2, 1)
        pos_col = pos_any.transpose(0, 2, 1)
        gate_here = jnp.sum(jnp.where(here, gates, 0.0), axis=1)
        gate_there = jnp.sum(jnp.where(there, gates, 0.0), axis=1)
        coef = jnp.where((cnt == 2)[:, None], gates, 1.0).transpose(0, 2, 1)
        split = (cnt[2] == 1) & (cnt_p[2] == 1)
        far_coef = jnp.stack([jnp.where(split, gate_here[2], 1.0), jnp.where(split, gate_there[2], 1.0)], axis=1)
        a0 = jnp.where(cnt[0] == 2, 1.0, gate_here[0])
        a1 = jnp.where(cnt_p[0] == 2, 1.0, gate_there[0])
        gate_far = jnp.sum(jnp.where(here[0] | there[0], 0.0, gates[0]), axis=0)
        a2 = jnp.where(cnt[0] + cnt_p[0] == 0, 1.0, gate_far)
        own_coef = jnp.stack([a0, a1, a2], axis=1)

        parts = 2
        half = width // parts
        u_home = dispatch(pos[:2], sel_gate[:2], ([d_own], [d_par]), cap, True)
        x_home = dispatch(pos[:2], sel_gate[:2], (x_y, x_p), cap, False)
        h_h, da_h, db_h = both(x_home, u_home, w_up, w_lin, w_down)

        x_rem = dispatch(pos[2:], sel_gate[2:], (x_x, x_o), cap, False)
        a_r, b_r, h_r = forward(x_rem, w_up, w_lin)
        y_x = []
        for k in range(parts):
            y2, y3 = out_rows(two[2:], pos_tok[2:], coef[2:], h_r, w_down, k, parts)
            y3 = move(y3, 0, 1)
            y_x.append(move(merge([y2, y3], half, coef=far_coef), 0, 2))

        u_rem = dispatch(pos[2:], sel_gate[2:], (d_x, d_o), cap, True)
        da_r, db_r = backward(u_rem, w_down, a_r, b_r)
        dx_x = []
        for k in range(parts):
            r2, r3 = dx_rows(pos_col[2:], da_r, db_r, w_up, w_lin, k, parts)
            r3 = move(r3, 0, 1)
            dx_x.append(move(merge([r2, r3], half), 0, 2))

        r0, r1 = dx_rows(pos_col[:2], da_h, db_h, w_up, w_lin, 0, 1)
        r1 = move(r1, 0, 1)
        dx_out = [move(merge([r0, r1, dx_x[k]], half, part=k), -1, 0) for k in range(parts)]
        dx_prev = jnp.concatenate(dx_out, axis=1)

        y0, y1 = out_rows(two[:2], pos_tok[:2], coef[:2], h_h, w_down, 0, 1)
        y1 = move(y1, 0, 1)
        y_tok = merge([y0, y1, *y_x], width, coef=own_coef, halves=parts)

        g_up, g_lin = grads_in(x_home, x_rem, da_h, da_r, db_h, db_r)
        g_down = grad_down(h_h, h_r, u_home, u_rem)
        return y_tok[None], dx_prev[None], g_up[None], g_lin[None], g_down[None]

    return jax.shard_map(device_step, mesh=mesh, in_specs=(tok_spec, tok_spec, tok_spec, w_spec, w_spec, w_spec, tok_spec), out_specs=(tok_spec, tok_spec, w_spec, w_spec, w_spec), check_vma=False)
```
